32 devices in a mesh: wide: 8 (over z, core), narrow: 4 (over y, x).
Axes of the slice: x: 2, y: 2, z: 4, core: 2. Of those that a mesh axis runs over, the one named last changes fastest.
Arguments:
- operator: bfloat16 [8, 4, 2, 2048, 2048], P('wide', 'narrow'), may hold values from -0.125 to 0.125
- sources: bfloat16 [8, 4, 2048, 128], P('wide', 'narrow'), may hold values from -6 to 6
- face_lengths: int32 [8, 4, 4], P('wide', 'narrow'), may hold values from 192 to 640, as said below
Outputs:
- outgoing: bfloat16 [8, 4, 2048, 128], P('wide', 'narrow')
- incoming: bfloat16 [8, 4, 2048, 128], P('wide', 'narrow')
The draws below stay inside these ranges and needn't reach their ends.
Inputs may be any that keep to these rules, and one draw needn't show every extreme that they name: `face_lengths`: the entries of adjacent subdomains for their common face are equal; lower-row and higher-row entries lie in 320 to 640, column entries in 192 to 384.
All inputs are finite; a program needn't handle non-finite values.
Results may differ from the reference program's by a relative error of at most 0.0055.
Values may be sent and summed in bfloat16 or wider, within the bound.
A program may use at most 64 MiB of HBM per device.

```python
import jax
import jax.numpy as jnp
from jax import lax

FACE_LONG = 640
FACE_SHORT = 384
SOURCES = 64
ITERS = 3
MMAX = 2048
SUB_ROWS = 8
SUB_COLS = 4


def draw_face_lengths(key, part):
    first_key, second_key = jax.random.split(jax.random.fold_in(key, 17))
    longs = jax.random.randint(first_key, (SUB_ROWS + 1, SUB_COLS), FACE_LONG // 2, FACE_LONG + 1)
    shorts = jax.random.randint(second_key, (SUB_ROWS, SUB_COLS + 1), FACE_SHORT // 2, FACE_SHORT + 1)
    longs = longs.at[0, 0].set(FACE_LONG).at[SUB_ROWS, SUB_COLS - 1].set(FACE_LONG // 2)
    shorts = shorts.at[0, 0].set(FACE_SHORT).at[SUB_ROWS - 1, SUB_COLS].set(FACE_SHORT // 2)
    stacked = jnp.stack([longs[:-1], longs[1:], shorts[:, :-1], shorts[:, 1:]], axis=-1)
    return stacked.astype(jnp.int32)


def block_scale(key, shape, pieces, smallest, top_value):
    def one(axis_at, shards_of):
        draws = jax.random.uniform(jax.random.fold_in(jax.random.fold_in(key, 6), axis_at), (shards_of,), jnp.float32, smallest / len(pieces), top_value / len(pieces))
        return jnp.repeat(jnp.exp(draws), shape[axis_at] // shards_of).reshape((-1,) + (1,) * (len(shape) - axis_at - 1))

    loudness = one(*pieces[0])
    for cut in pieces[1:]:
        loudness = loudness * one(*cut)
    return loudness


def centred(key, shape, scale, limit, shards=(), held_as=jnp.bfloat16):
    values = scale * jax.random.normal(key, shape, jnp.float32)
    if shards:
        values = values * block_scale(key, shape, shards, -0.22, 0.18)
    return jnp.clip(values, -limit, limit).astype(held_as)


def setup_inputs(seed: int = 0) -> dict:
    splits = jax.random.split(jax.random.key(seed), 4)
    return {
        "operator": centred(splits[0], (SUB_ROWS, SUB_COLS, 2, MMAX, MMAX), MMAX ** -0.5, 0.125, ((0, 8), (1, 4))),
        "sources": centred(splits[1], (SUB_ROWS, SUB_COLS, MMAX, 2 * SOURCES), 1.0, 6.0, ((0, 8), (1, 4))),
        "face_lengths": draw_face_lengths(jax.random.fold_in(splits[3], 71), 0),
    }


def live_rows(counts):
    total = 2 * FACE_LONG + 2 * FACE_SHORT
    rows = jnp.arange(total, dtype=jnp.int32)
    edges = [0, FACE_LONG, 2 * FACE_LONG, 2 * FACE_LONG + FACE_SHORT]
    live = jnp.zeros((total,), dtype=bool)
    for face in range(4):
        live = live | ((rows >= edges[face]) & (rows < edges[face] + counts[face]))
    return live[:, None]


def trade_all(out):
    low = FACE_LONG
    mid = 2 * FACE_LONG
    high = 2 * FACE_LONG + FACE_SHORT
    lower_face = out[:, :, :low]
    upper_face = out[:, :, low:mid]
    left_face = out[:, :, mid:high]
    right_face = out[:, :, high:]
    zero_row = jnp.zeros_like(upper_face[:1])
    from_lower = jnp.concatenate([zero_row, upper_face[:-1]], axis=0)
    from_upper = jnp.concatenate([lower_face[1:], zero_row], axis=0)
    zero_col = jnp.zeros_like(right_face[:, :1])
    from_left = jnp.concatenate([zero_col, right_face[:, :-1]], axis=1)
    from_right = jnp.concatenate([left_face[:, 1:], zero_col], axis=1)
    return jnp.concatenate([from_lower, from_upper, from_left, from_right], axis=2)


def product(pair):
    oper, field = pair
    total = oper.shape[-1]
    half = field.shape[1] // 2
    stacked = oper.reshape(2 * total, total).astype(jnp.float32)
    both = jnp.dot(stacked, field.astype(jnp.float32), precision=lax.Precision.HIGHEST)
    first = both[:total]
    second = both[total:]
    real_part = first[:, :half] - second[:, half:]
    imag_part = first[:, half:] + second[:, :half]
    return jnp.concatenate([real_part, imag_part], axis=1)


def reference(operator, sources, face_lengths):
    rows_grid, cols_grid = operator.shape[0], operator.shape[1]
    total = operator.shape[-1]
    width = sources.shape[-1]
    count = rows_grid * cols_grid
    live = jax.vmap(live_rows)(face_lengths.reshape(count, 4)).reshape(rows_grid, cols_grid, total, 1)
    masked = jnp.where(live, sources, jnp.zeros_like(sources))
    incoming = trade_all(masked)
    oper_flat = operator.reshape(count, 2, total, total)
    outgoing = masked
    for step in range(ITERS):
        terms = lax.map(product, (oper_flat, incoming.reshape(count, total, width)))
        terms = terms.reshape(rows_grid, cols_grid, total, width) + sources.astype(jnp.float32)
        outgoing = jnp.where(live, terms, jnp.zeros_like(terms)).astype(jnp.bfloat16)
        incoming = trade_all(outgoing)
    return outgoing, incoming
```

```python
import functools

import jax
import jax.numpy as jnp
from jax import lax
from jax.experimental import pallas as pl
from jax.experimental.pallas import tpu as pltpu
from jax.sharding import PartitionSpec as P

FACE_LONG = 640
FACE_SHORT = 384
ITERS = 3
CHUNK = 128
EARLY = 3
MESH = pl.DeviceIdType.MESH


def kernel(n_wide, n_narrow, oper_hbm, src_hbm, len_ref, last_out, last_in,
           stage, wt, src, src_t, landed, xs, acc, out_long, out_short,
           w_sem, src_sem, send_sem, recv_sem):
    total, width = src.shape
    half = width // 2
    short0 = 2 * FACE_LONG
    far_k, short_k = 2 * FACE_LONG, 4 * FACE_LONG
    far_n, near_n = 2 * FACE_SHORT, 2 * FACE_SHORT + FACE_LONG
    chunks = total // CHUNK
    row = lax.axis_index("wide")
    col = lax.axis_index("narrow")
    far = lax.rem(row, 2)
    near = 1 - far
    first = jnp.where(2 * col < n_narrow, 1, 0)
    second = 1 - first

    def long_off(face):
        return pl.multiple_of(face * FACE_LONG, 128)

    def short_off(face):
        return pl.multiple_of(short0 + face * FACE_SHORT, 128)

    faces = [(False, first, None), (False, second, None), (True, far, 1), (True, near, 0)]

    def geometry(is_long, face):
        if is_long:
            target = row + 2 * face - 1
            return (long_off(face), long_off(1 - face), FACE_LONG, {"wide": target},
                    (target >= 0) & (target < n_wide), face, 1 - face)
        target = col + 2 * face - 1
        return (short_off(face), short_off(1 - face), FACE_SHORT, {"narrow": target},
                (target >= 0) & (target < n_narrow), 2 + face, 3 - face)

    def k_off(is_long, face, role):
        if is_long:
            return role * far_k
        return pl.multiple_of(short_k + face * 2 * FACE_SHORT, 128)

    def ends(step, is_long, face, role, sending):
        here, there, size, device, exists, slot, other = geometry(is_long, face)
        if step in (0, ITERS):
            source = (src if step == 0 else last_out).at[pl.ds(here, size)]
            target = (landed if step == 0 else last_in).at[pl.ds(there if sending else here, size)]
        else:
            source = out_long.at[step - 1, role] if is_long else out_short.at[step - 1, face]
            at = k_off(is_long, 1 - face if sending else face, role)
            target = xs.at[step, :, pl.ds(at, size)]
        copy = pltpu.make_async_remote_copy(
            src_ref=source,
            dst_ref=target,
            send_sem=send_sem.at[step, slot],
            recv_sem=recv_sem.at[step, other if sending else slot],
            device_id=device,
            device_id_type=MESH,
        )
        return copy, exists

    def send(step, is_long, face, role, start):
        copy, exists = ends(step, is_long, face, role, True)

        @pl.when(exists)
        def _():
            if start:
                copy.start()
            else:
                copy.wait_send()

    def receive(step, is_long, face, role):
        copy, exists = ends(step, is_long, face, role, False)

        @pl.when(exists)
        def _():
            copy.wait_recv()

    src_copy = pltpu.make_async_copy(src_hbm.at[0, 0], src, src_sem)
    src_copy.start()

    barrier = pltpu.get_barrier_semaphore()
    count = jnp.int32(0)
    for is_long, face, _ in faces:
        _, _, _, device, exists, _, _ = geometry(is_long, face)
        count = count + exists.astype(jnp.int32)

        @pl.when(exists)
        def _():
            pl.semaphore_signal(barrier, inc=1, device_id=device, device_id_type=MESH)

    def load(n):
        shorts = far_n // CHUNK
        longs = FACE_LONG // CHUNK
        at = jnp.where(n < shorts, short0 + n * CHUNK,
                       jnp.where(n < shorts + longs, far * FACE_LONG + (n - shorts) * CHUNK,
                                 near * FACE_LONG + (n - shorts - longs) * CHUNK))
        return pltpu.make_async_copy(
            oper_hbm.at[0, 0, :, pl.ds(pl.multiple_of(at, CHUNK), CHUNK), :],
            stage.at[n], w_sem.at[n])

    @pl.loop(0, EARLY)
    def _(n):
        load(n).start()

    src_copy.wait()
    pl.semaphore_wait(barrier, count)
    for face in faces:
        send(0, *face, True)

    @pl.loop(EARLY, chunks)
    def _(n):
        load(n).start()

    def live(slot, shape):
        return lax.broadcasted_iota(jnp.int32, shape, 1) < len_ref[0, 0, slot]

    def masked(value, slot):
        return jnp.where(live(slot, value.shape), value, 0.0)

    for is_long, face, role in faces:
        here, _, size, _, exists, _, _ = geometry(is_long, face)

        @pl.when(jnp.logical_not(exists))
        def _():
            landed[pl.ds(here, size), :] = jnp.zeros((size, width), landed.dtype)
            last_in[pl.ds(here, size), :] = jnp.zeros((size, width), last_in.dtype)
            for step in range(1, ITERS):
                xs[step, :, pl.ds(k_off(is_long, face, role), size)] = jnp.zeros((width, size), xs.dtype)

    src_t[:, pl.ds(0, far_n)] = src[pl.ds(short0, far_n), :].T
    src_t[:, pl.ds(far_n, FACE_LONG)] = src[pl.ds(long_off(far), FACE_LONG), :].T
    src_t[:, pl.ds(near_n, FACE_LONG)] = src[pl.ds(long_off(near), FACE_LONG), :].T

    blocks = [(long_off(near), FACE_LONG, 0), (long_off(far), FACE_LONG, far_k),
              (short0, FACE_SHORT, short_k), (short0 + FACE_SHORT, FACE_SHORT, short_k + 2 * FACE_SHORT)]

    @pl.loop(0, chunks)
    def _(n):
        load(n).wait()
        cols = pl.ds(pl.multiple_of(n * CHUNK, CHUNK), CHUNK)
        for part in range(2):
            for at, size, k in blocks:
                wt[pl.ds(k + part * size, size), cols] = stage[n, part, :, pl.ds(at, size)].T

    def prepare(step, is_long, face, role):
        here, _, size, _, _, slot, _ = geometry(is_long, face)
        at = k_off(is_long, face, role)
        if step == 0:
            value = masked(landed[pl.ds(here, size), :].T.astype(jnp.float32), slot).astype(xs.dtype)
            xs[step, :, pl.ds(at, size)] = value
        else:
            value = xs[step, :, pl.ds(at, size)]
        turned = jnp.concatenate([-value[half:], value[:half]], axis=0)
        xs[step, :, pl.ds(pl.multiple_of(at + size, 128), size)] = turned

    def product(step, k, depth, n, cols):
        return jnp.dot(xs[step, :, pl.ds(k, depth)], wt[pl.ds(k, depth), pl.ds(n, cols)],
                       preferred_element_type=jnp.float32)

    def finish(step, is_long, face, role, value):
        here, _, size, _, _, slot, _ = geometry(is_long, face)
        value = masked(value, slot).astype(xs.dtype)
        if step == ITERS:
            last_out[pl.ds(here, size), :] = value.T
        elif is_long:
            out_long[step - 1, role] = value
        else:
            out_short[step - 1, face] = value

    for step in range(ITERS):
        for face, role in ((near, 0), (far, 1)):
            receive(step, True, face, role)
            prepare(step, True, face, role)
            for n in range(0, total, 512):
                base = src_t[:, pl.ds(n, 512)].astype(jnp.float32) if role == 0 else acc[:, pl.ds(n, 512)]
                acc[:, pl.ds(n, 512)] = base + product(step, role * far_k, far_k, n, 512)
        for face in (second, first):
            receive(step, False, face, None)
        for face in (0, 1):
            prepare(step, False, face, None)
        depth = 4 * FACE_SHORT
        value = acc[:, pl.ds(0, far_n)] + product(step, short_k, depth, 0, far_n)
        for face in (0, 1):
            finish(step + 1, False, face, None, value[:, face * FACE_SHORT:(face + 1) * FACE_SHORT])
        send(step + 1, *faces[0], True)
        send(step + 1, *faces[1], True)
        value = acc[:, pl.ds(far_n, 768)] + product(step, short_k, depth, far_n, 768)
        finish(step + 1, True, far, 1, value[:, :FACE_LONG])
        send(step + 1, *faces[2], True)
        rest = acc[:, pl.ds(far_n + 768, 512)] + product(step, short_k, depth, far_n + 768, 512)
        finish(step + 1, True, near, 0, jnp.concatenate([value[:, FACE_LONG:], rest], axis=1))
        send(step + 1, *faces[3], True)

    for step in range(ITERS + 1):
        for face in faces:
            send(step, *face, False)
    for face in faces[::-1]:
        receive(ITERS, *face)


def write_out(out_ref, in_ref, out_hbm, in_hbm, sem):
    copies = [pltpu.make_async_copy(out_ref, out_hbm.at[0, 0], sem.at[0]),
              pltpu.make_async_copy(in_ref, in_hbm.at[0, 0], sem.at[1])]
    for copy in copies:
        copy.start()
    for copy in copies:
        copy.wait()


def body(n_wide, n_narrow, operator, sources, face_lengths):
    total, width = sources.shape[2:]
    dtype = sources.dtype
    held = pltpu.VMEM((total, width), dtype)
    outgoing, incoming = pl.pallas_call(
        functools.partial(kernel, n_wide, n_narrow),
        out_shape=(held, held),
        in_specs=[
            pl.BlockSpec(memory_space=pltpu.HBM),
            pl.BlockSpec(memory_space=pltpu.HBM),
            pl.BlockSpec(memory_space=pltpu.SMEM),
        ],
        out_specs=[pl.BlockSpec(memory_space=pltpu.VMEM)] * 2,
        scratch_shapes=[
            pltpu.VMEM((total // CHUNK, 2, CHUNK, total), dtype),
            pltpu.VMEM((2 * total, total), dtype),
            pltpu.VMEM((total, width), dtype),
            pltpu.VMEM((width, total), dtype),
            pltpu.VMEM((total, width), dtype),
            pltpu.VMEM((ITERS, width, 2 * total), dtype),
            pltpu.VMEM((width, total), jnp.float32),
            pltpu.VMEM((ITERS - 1, 2, width, FACE_LONG), dtype),
            pltpu.VMEM((ITERS - 1, 2, width, FACE_SHORT), dtype),
            pltpu.SemaphoreType.DMA((total // CHUNK,)),
            pltpu.SemaphoreType.DMA,
            pltpu.SemaphoreType.DMA((ITERS + 1, 4)),
            pltpu.SemaphoreType.DMA((ITERS + 1, 4)),
        ],
        compiler_params=pltpu.CompilerParams(
            collective_id=0, has_side_effects=True, vmem_limit_bytes=54 * 1024 * 1024),
        name="schwarz",
    )(operator, sources, face_lengths)
    shape = jax.ShapeDtypeStruct(sources.shape, dtype)
    return pl.pallas_call(
        write_out,
        out_shape=(shape, shape),
        in_specs=[pl.BlockSpec(memory_space=pltpu.VMEM)] * 2,
        out_specs=[pl.BlockSpec(memory_space=pl.ANY)] * 2,
        scratch_shapes=[pltpu.SemaphoreType.DMA((2,))],
        compiler_params=pltpu.CompilerParams(vmem_limit_bytes=4 * 1024 * 1024),
        name="write_out",
    )(outgoing, incoming)


def solution(mesh):
    in_specs = (
        P("wide", "narrow", None, None, None),
        P("wide", "narrow", None, None),
        P("wide", "narrow", None),
    )
    out_specs = (P("wide", "narrow", None, None), P("wide", "narrow", None, None))
    step = functools.partial(body, mesh.shape["wide"], mesh.shape["narrow"])
    return jax.shard_map(step, mesh=mesh, in_specs=in_specs, out_specs=out_specs, check_vma=False)
```

```python
import functools

import jax
import jax.numpy as jnp
from jax import lax
from jax.experimental import pallas as pl
from jax.experimental.pallas import tpu as pltpu
from jax.sharding import PartitionSpec as P

FACE_LONG = 640
FACE_SHORT = 384
ITERS = 3
CHUNK = 128
EARLY = 8
WIDE = 256
MESH = pl.DeviceIdType.MESH


def kernel(n_wide, n_narrow, oper_hbm, src_hbm, len_hbm, last_out, last_in,
           stage, wt, src, src_t, landed, xs, acc, out_long, out_short, lens,
           w_sem, src_sem, len_sem, send_sem, recv_sem):
    total, width = src.shape
    half = width // 2
    short0 = 2 * FACE_LONG
    far_n, near_n = 2 * FACE_SHORT, 2 * FACE_SHORT + FACE_LONG
    long_k, short_k = 2 * FACE_LONG, 2 * FACE_SHORT
    near_k, second_k, far_k, first_k = 0, long_k, long_k + short_k, 2 * long_k + short_k
    chunks = total // CHUNK
    row = lax.axis_index("wide")
    col = lax.axis_index("narrow")
    far = lax.rem(row, 2)
    near = 1 - far

    def inward(at):
        return jnp.where(2 * at < n_narrow, 1, 0)

    first = inward(col)
    second = 1 - first

    def long_off(face):
        return pl.multiple_of(face * FACE_LONG, 128)

    def short_off(face):
        return pl.multiple_of(short0 + face * FACE_SHORT, 128)

    faces = [(False, first, first_k), (False, second, second_k), (True, far, far_k), (True, near, near_k)]

    def geometry(is_long, face):
        if is_long:
            target = row + 2 * face - 1
            return (long_off(face), long_off(1 - face), FACE_LONG, {"wide": target},
                    (target >= 0) & (target < n_wide), face, 1 - face)
        target = col + 2 * face - 1
        return (short_off(face), short_off(1 - face), FACE_SHORT, {"narrow": target},
                (target >= 0) & (target < n_narrow), 2 + face, 3 - face)

    def ends(step, is_long, face, k, sending):
        here, there, size, device, exists, slot, other = geometry(is_long, face)
        if step in (0, ITERS):
            source = (src if step == 0 else last_out).at[pl.ds(here, size)]
            target = (landed if step == 0 else last_in).at[pl.ds(there if sending else here, size)]
        else:
            source = out_long.at[step - 1, int(k == far_k)] if is_long else out_short.at[step - 1, face]
            if sending and not is_long:
                k = pl.multiple_of(jnp.where(1 - face == inward(col + 2 * face - 1), first_k, second_k), 128)
            target = xs.at[step, :, pl.ds(k, size)]
        copy = pltpu.make_async_remote_copy(
            src_ref=source,
            dst_ref=target,
            send_sem=send_sem.at[step, slot],
            recv_sem=recv_sem.at[step, other if sending else slot],
            device_id=device,
            device_id_type=MESH,
        )
        return copy, exists

    def send(step, is_long, face, k, start):
        copy, exists = ends(step, is_long, face, k, True)

        @pl.when(exists)
        def _():
            if start:
                copy.start()
            else:
                copy.wait_send()

    def receive(step, is_long, face, k):
        copy, exists = ends(step, is_long, face, k, False)

        @pl.when(exists)
        def _():
            copy.wait_recv()

    src_copy = pltpu.make_async_copy(src_hbm.at[0, 0], src, src_sem)
    src_copy.start()
    len_copy = pltpu.make_async_copy(len_hbm.at[0, 0], lens, len_sem)
    len_copy.start()

    barrier = pltpu.get_barrier_semaphore()
    count = jnp.int32(0)
    for is_long, face, _ in faces:
        _, _, _, device, exists, _, _ = geometry(is_long, face)
        count = count + exists.astype(jnp.int32)

        @pl.when(exists)
        def _():
            pl.semaphore_signal(barrier, inc=1, device_id=device, device_id_type=MESH)

    def load(n):
        shorts = far_n // CHUNK
        longs = FACE_LONG // CHUNK
        at = jnp.where(n < shorts, short0 + n * CHUNK,
                       jnp.where(n < shorts + longs, far * FACE_LONG + (n - shorts) * CHUNK,
                                 near * FACE_LONG + (n - shorts - longs) * CHUNK))
        return pltpu.make_async_copy(
            oper_hbm.at[0, 0, :, pl.ds(pl.multiple_of(at, CHUNK), CHUNK), :],
            stage.at[:, pl.ds(pl.multiple_of(n * CHUNK, CHUNK), CHUNK), :], w_sem.at[n])

    @pl.loop(0, EARLY)
    def _(n):
        load(n).start()

    src_copy.wait()
    pl.semaphore_wait(barrier, count)
    for face in faces:
        send(0, *face, True)

    @pl.loop(EARLY, chunks)
    def _(n):
        load(n).start()

    len_copy.wait()

    def masked(value, slot):
        slots = lax.broadcasted_iota(jnp.int32, value.shape, 1)
        return jnp.where(slots < lens[slot], value, 0.0)

    for is_long, face, k in faces:
        here, _, size, _, exists, _, _ = geometry(is_long, face)

        @pl.when(jnp.logical_not(exists))
        def _():
            landed[pl.ds(here, size), :] = jnp.zeros((size, width), landed.dtype)
            last_in[pl.ds(here, size), :] = jnp.zeros((size, width), last_in.dtype)
            for step in range(1, ITERS):
                xs[step, :, pl.ds(k, size)] = jnp.zeros((width, size), xs.dtype)

    src_t[:, pl.ds(0, far_n)] = src[pl.ds(short0, far_n), :].T
    src_t[:, pl.ds(far_n, FACE_LONG)] = src[pl.ds(long_off(far), FACE_LONG), :].T
    src_t[:, pl.ds(near_n, FACE_LONG)] = src[pl.ds(long_off(near), FACE_LONG), :].T

    blocks = [(long_off(near), FACE_LONG, near_k), (long_off(far), FACE_LONG, far_k),
              (short_off(second), FACE_SHORT, second_k), (short_off(first), FACE_SHORT, first_k)]

    def turn(n, which):
        for part in range(2):
            for at, size, k in which:
                wt[pl.ds(k + part * size, size), pl.ds(n * CHUNK, CHUNK)] = (
                    stage[part, pl.ds(n * CHUNK, CHUNK), pl.ds(at, size)].T)

    def arrive(step, is_long, face, k):
        receive(step, is_long, face, k)
        here, _, size, _, _, slot, _ = geometry(is_long, face)
        if step == 0:
            value = masked(landed[pl.ds(here, size), :].T.astype(jnp.float32), slot).astype(xs.dtype)
            xs[step, :, pl.ds(k, size)] = value
        else:
            value = xs[step, :, pl.ds(k, size)]
        xs[step, :, pl.ds(k + size, size)] = jnp.concatenate([-value[half:], value[:half]], axis=0)

    def product(step, k, depth, n, cols):
        return jnp.dot(xs[step, :, pl.ds(k, depth)], wt[pl.ds(k, depth), pl.ds(n, cols)],
                       preferred_element_type=jnp.float32)

    def add(step, k, depth, n, cols):
        base = src_t[:, pl.ds(n, cols)].astype(jnp.float32) if k == near_k else acc[:, pl.ds(n, cols)]
        acc[:, pl.ds(n, cols)] = base + product(step, k, depth, n, cols)

    def add_unturned(n):
        value = src_t[:, pl.ds(n, WIDE)].astype(jnp.float32)
        for part in range(2):
            value = value + lax.dot_general(
                xs[0, :, pl.ds(near_k + part * FACE_LONG, FACE_LONG)],
                stage[part, pl.ds(n, WIDE), pl.ds(long_off(near), FACE_LONG)],
                (((1,), (1,)), ((), ())), preferred_element_type=jnp.float32)
        acc[:, pl.ds(n, WIDE)] = value

    def finish(step, is_long, face, k, n):
        here, _, size, _, _, slot, _ = geometry(is_long, face)
        value = masked(acc[:, pl.ds(n, size)], slot).astype(xs.dtype)
        if step == ITERS:
            last_out[pl.ds(here, size), :] = value.T
        elif is_long:
            out_long[step - 1, int(k == far_k)] = value
        else:
            out_short[step - 1, face] = value

    def finish_shorts(step):
        for face in (0, 1):
            finish(step, False, face, None, face * FACE_SHORT)
        for face in faces[:2]:
            send(step, *face, True)

    def finish_far(step):
        finish(step, *faces[2], far_n)
        send(step, *faces[2], True)

    wide = 2 * FACE_SHORT

    for step in range(ITERS):
        if step == 0:
            per = WIDE // CHUNK
            groups = chunks // per
            for group in range(groups):
                if group == groups // 2:
                    arrive(0, *faces[3])
                for n in range(group * per, group * per + per):
                    load(n).wait()
                    turn(n, blocks[1:])
                if group >= groups // 2:
                    for g in range(2 * (group - groups // 2), 2 * (group - groups // 2) + 2):
                        add_unturned(g * WIDE)
        else:
            arrive(step, *faces[3])
            for n in range(0, total, WIDE):
                add(step, near_k, long_k, n, WIDE)
            for face in faces:
                send(step - 1, *face, False)
        arrive(step, *faces[1])
        add(step, second_k, short_k, 0, wide)
        arrive(step, *faces[2])
        add(step, far_k, long_k, 0, wide)
        arrive(step, *faces[0])
        add(step, first_k, short_k, 0, wide)
        finish_shorts(step + 1)
        add(step, second_k, long_k + 2 * short_k, wide, wide)
        finish_far(step + 1)
        add(step, second_k, long_k + 2 * short_k, 2 * wide, total - 2 * wide)
        finish(step + 1, *faces[3], near_n)
        send(step + 1, *faces[3], True)
        if step == 0:
            for n in range(chunks):
                turn(n, blocks[:1])

    for step in (ITERS - 1, ITERS):
        for face in faces:
            send(step, *face, False)
    for face in faces[::-1]:
        receive(ITERS, *face)


def write_out(out_ref, in_ref, out_hbm, in_hbm, sem):
    copies = [pltpu.make_async_copy(out_ref, out_hbm.at[0, 0], sem.at[0]),
              pltpu.make_async_copy(in_ref, in_hbm.at[0, 0], sem.at[1])]
    for copy in copies:
        copy.start()
    for copy in copies:
        copy.wait()


def body(n_wide, n_narrow, operator, sources, face_lengths):
    total, width = sources.shape[2:]
    dtype = sources.dtype
    held = pltpu.VMEM((total, width), dtype)
    outgoing, incoming = pl.pallas_call(
        functools.partial(kernel, n_wide, n_narrow),
        out_shape=(held, held),
        in_specs=[
            pl.BlockSpec(memory_space=pltpu.HBM),
            pl.BlockSpec(memory_space=pltpu.HBM),
            pl.BlockSpec(memory_space=pltpu.HBM),
        ],
        out_specs=[pl.BlockSpec(memory_space=pltpu.VMEM)] * 2,
        scratch_shapes=[
            pltpu.VMEM((2, total, total), dtype),
            pltpu.VMEM((2 * total, total), dtype),
            pltpu.VMEM((total, width), dtype),
            pltpu.VMEM((width, total), dtype),
            pltpu.VMEM((total, width), dtype),
            pltpu.VMEM((ITERS, width, 2 * total), dtype),
            pltpu.VMEM((width, total), jnp.float32),
            pltpu.VMEM((ITERS - 1, 2, width, FACE_LONG), dtype),
            pltpu.VMEM((ITERS - 1, 2, width, FACE_SHORT), dtype),
            pltpu.SMEM((4,), jnp.int32),
            pltpu.SemaphoreType.DMA((total // CHUNK,)),
            pltpu.SemaphoreType.DMA,
            pltpu.SemaphoreType.DMA,
            pltpu.SemaphoreType.DMA((ITERS + 1, 4)),
            pltpu.SemaphoreType.DMA((ITERS + 1, 4)),
        ],
        compiler_params=pltpu.CompilerParams(
            collective_id=0, has_side_effects=True, vmem_limit_bytes=54 * 1024 * 1024),
        name="schwarz",
    )(operator, sources, face_lengths)
    shape = jax.ShapeDtypeStruct(sources.shape, dtype)
    return pl.pallas_call(
        write_out,
        out_shape=(shape, shape),
        in_specs=[pl.BlockSpec(memory_space=pltpu.VMEM)] * 2,
        out_specs=[pl.BlockSpec(memory_space=pl.ANY)] * 2,
        scratch_shapes=[pltpu.SemaphoreType.DMA((2,))],
        compiler_params=pltpu.CompilerParams(vmem_limit_bytes=4 * 1024 * 1024),
        name="write_out",
    )(outgoing, incoming)


def solution(mesh):
    in_specs = (
        P("wide", "narrow", None, None, None),
        P("wide", "narrow", None, None),
        P("wide", "narrow", None),
    )
    out_specs = (P("wide", "narrow", None, None), P("wide", "narrow", None, None))
    step = functools.partial(body, mesh.shape["wide"], mesh.shape["narrow"])
    return jax.shard_map(step, mesh=mesh, in_specs=in_specs, out_specs=out_specs, check_vma=False)
```

```python
import functools

import jax
import jax.numpy as jnp
from jax import lax
from jax.experimental import pallas as pl
from jax.experimental.pallas import tpu as pltpu
from jax.sharding import PartitionSpec as P

FACE_LONG = 640
FACE_SHORT = 384
ITERS = 3
CHUNK = 128
EARLY = 8
WIDE = 256
MESH = pl.DeviceIdType.MESH


def kernel(n_wide, n_narrow, oper_hbm, src_hbm, len_hbm, last_out, last_in,
           stage, wt, src, src_t, landed, xs, acc, out_long, out_short, lens,
           w_sem, src_sem, len_sem, send_sem, recv_sem):
    total, width = src.shape
    half = width // 2
    short0 = 2 * FACE_LONG
    far_n, near_n = 2 * FACE_SHORT, 2 * FACE_SHORT + FACE_LONG
    long_k, short_k = 2 * FACE_LONG, 2 * FACE_SHORT
    near_k, second_k, far_k, first_k = 0, long_k, long_k + short_k, 2 * long_k + short_k
    chunks = total // CHUNK
    row = lax.axis_index("wide")
    col = lax.axis_index("narrow")
    far = lax.rem(row, 2)
    near = 1 - far

    def inward(at):
        return jnp.where(2 * at < n_narrow, 1, 0)

    first = inward(col)
    second = 1 - first

    def long_off(face):
        return pl.multiple_of(face * FACE_LONG, 128)

    def short_off(face):
        return pl.multiple_of(short0 + face * FACE_SHORT, 128)

    faces = [(False, first, first_k), (False, second, second_k), (True, far, far_k), (True, near, near_k)]

    def geometry(is_long, face):
        if is_long:
            target = row + 2 * face - 1
            return (long_off(face), long_off(1 - face), FACE_LONG, {"wide": target},
                    (target >= 0) & (target < n_wide), face, 1 - face)
        target = col + 2 * face - 1
        return (short_off(face), short_off(1 - face), FACE_SHORT, {"narrow": target},
                (target >= 0) & (target < n_narrow), 2 + face, 3 - face)

    def ends(step, is_long, face, k, sending):
        here, there, size, device, exists, slot, other = geometry(is_long, face)
        if step in (0, ITERS):
            source = (src if step == 0 else last_out).at[pl.ds(here, size)]
            target = (landed if step == 0 else last_in).at[pl.ds(there if sending else here, size)]
        else:
            source = out_long.at[step - 1, int(k == far_k)] if is_long else out_short.at[step - 1, face]
            if sending and not is_long:
                k = pl.multiple_of(jnp.where(1 - face == inward(col + 2 * face - 1), first_k, second_k), 128)
            target = xs.at[step, :, pl.ds(k, size)]
        copy = pltpu.make_async_remote_copy(
            src_ref=source,
            dst_ref=target,
            send_sem=send_sem.at[step, slot],
            recv_sem=recv_sem.at[step, other if sending else slot],
            device_id=device,
            device_id_type=MESH,
        )
        return copy, exists

    def send(step, is_long, face, k, start, also=True):
        copy, exists = ends(step, is_long, face, k, True)

        @pl.when(exists & also)
        def _():
            if start:
                copy.start()
            else:
                copy.wait_send()

    def receive(step, is_long, face, k):
        copy, exists = ends(step, is_long, face, k, False)

        @pl.when(exists)
        def _():
            copy.wait_recv()

    src_copy = pltpu.make_async_copy(src_hbm.at[0, 0], src, src_sem)
    src_copy.start()
    len_copy = pltpu.make_async_copy(len_hbm.at[0, 0], lens, len_sem)
    len_copy.start()

    barrier = pltpu.get_barrier_semaphore()
    count = jnp.int32(0)
    for is_long, face, _ in faces:
        _, _, _, device, exists, _, _ = geometry(is_long, face)
        count = count + exists.astype(jnp.int32)

        @pl.when(exists)
        def _():
            pl.semaphore_signal(barrier, inc=1, device_id=device, device_id_type=MESH)

    def load(n):
        shorts = far_n // CHUNK
        longs = FACE_LONG // CHUNK
        half_way = shorts // 2
        at = jnp.where(n < shorts, short0 + jnp.where(n < half_way, first * FACE_SHORT + n * CHUNK,
                                                      second * FACE_SHORT + (n - half_way) * CHUNK),
                       jnp.where(n < shorts + longs, far * FACE_LONG + (n - shorts) * CHUNK,
                                 near * FACE_LONG + (n - shorts - longs) * CHUNK))
        return pltpu.make_async_copy(
            oper_hbm.at[0, 0, :, pl.ds(pl.multiple_of(at, CHUNK), CHUNK), :],
            stage.at[:, pl.ds(pl.multiple_of(n * CHUNK, CHUNK), CHUNK), :], w_sem.at[n])

    @pl.loop(0, EARLY)
    def _(n):
        load(n).start()

    src_copy.wait()
    pl.semaphore_wait(barrier, count)
    for face in faces[:2]:
        send(0, *face, True, far == 0)
    for face in faces[2:]:
        send(0, *face, True)

    @pl.loop(EARLY, chunks)
    def _(n):
        load(n).start()

    len_copy.wait()

    def masked(value, slot):
        slots = lax.broadcasted_iota(jnp.int32, value.shape, 1)
        return jnp.where(slots < lens[slot], value, 0.0)

    for is_long, face, k in faces:
        here, _, size, _, exists, _, _ = geometry(is_long, face)

        @pl.when(jnp.logical_not(exists))
        def _():
            landed[pl.ds(here, size), :] = jnp.zeros((size, width), landed.dtype)
            last_in[pl.ds(here, size), :] = jnp.zeros((size, width), last_in.dtype)
            for step in range(1, ITERS):
                xs[step, :, pl.ds(k, size)] = jnp.zeros((width, size), xs.dtype)

    src_t[:, pl.ds(0, FACE_SHORT)] = src[pl.ds(short_off(first), FACE_SHORT), :].T
    src_t[:, pl.ds(FACE_SHORT, FACE_SHORT)] = src[pl.ds(short_off(second), FACE_SHORT), :].T
    src_t[:, pl.ds(far_n, FACE_LONG)] = src[pl.ds(long_off(far), FACE_LONG), :].T
    src_t[:, pl.ds(near_n, FACE_LONG)] = src[pl.ds(long_off(near), FACE_LONG), :].T

    for face in faces[:2]:
        send(0, *face, True, far == 1)

    blocks = [(long_off(near), FACE_LONG, near_k), (long_off(far), FACE_LONG, far_k),
              (short_off(second), FACE_SHORT, second_k), (short_off(first), FACE_SHORT, first_k)]

    def turn(n, which):
        for part in range(2):
            for at, size, k in which:
                wt[pl.ds(k + part * size, size), pl.ds(n * CHUNK, CHUNK)] = (
                    stage[part, pl.ds(n * CHUNK, CHUNK), pl.ds(at, size)].T)

    def arrive(step, is_long, face, k):
        receive(step, is_long, face, k)
        here, _, size, _, _, slot, _ = geometry(is_long, face)
        if step == 0:
            value = masked(landed[pl.ds(here, size), :].T.astype(jnp.float32), slot).astype(xs.dtype)
            xs[step, :, pl.ds(k, size)] = value
        else:
            value = xs[step, :, pl.ds(k, size)]
        xs[step, :, pl.ds(k + size, size)] = jnp.concatenate([-value[half:], value[:half]], axis=0)

    def product(step, k, depth, n, cols):
        return jnp.dot(xs[step, :, pl.ds(k, depth)], wt[pl.ds(k, depth), pl.ds(n, cols)],
                       preferred_element_type=jnp.float32)

    def add(step, k, depth, n, cols):
        base = src_t[:, pl.ds(n, cols)].astype(jnp.float32) if k == near_k else acc[:, pl.ds(n, cols)]
        acc[:, pl.ds(n, cols)] = base + product(step, k, depth, n, cols)

    def add_unturned(n):
        value = src_t[:, pl.ds(n, WIDE)].astype(jnp.float32)
        for part in range(2):
            value = value + lax.dot_general(
                xs[0, :, pl.ds(near_k + part * FACE_LONG, FACE_LONG)],
                stage[part, pl.ds(n, WIDE), pl.ds(long_off(near), FACE_LONG)],
                (((1,), (1,)), ((), ())), preferred_element_type=jnp.float32)
        acc[:, pl.ds(n, WIDE)] = value

    def finish(step, is_long, face, k, value):
        here, _, size, _, _, slot, _ = geometry(is_long, face)
        value = masked(value, slot).astype(xs.dtype)
        if step == ITERS:
            last_out[pl.ds(here, size), :] = value.T
        elif is_long:
            out_long[step - 1, int(k == far_k)] = value
        else:
            out_short[step - 1, face] = value
        send(step, is_long, face, k, True)

    def closed(step, k, depth, n, cols):
        return acc[:, pl.ds(n, cols)] + product(step, k, depth, n, cols)

    wide = 2 * FACE_SHORT

    for step in range(ITERS):
        if step == 0:
            per = WIDE // CHUNK
            groups = chunks // per
            for group in range(groups):
                if group == groups // 2:
                    arrive(0, *faces[3])
                for n in range(group * per, group * per + per):
                    load(n).wait()
                    turn(n, blocks[1:])
                if group >= groups // 2:
                    for g in range(2 * (group - groups // 2), 2 * (group - groups // 2) + 2):
                        add_unturned(g * WIDE)
        else:
            arrive(step, *faces[3])
            for n in range(0, total, WIDE):
                add(step, near_k, long_k, n, WIDE)
            for face in faces:
                send(step - 1, *face, False)
        arrive(step, *faces[1])
        add(step, second_k, short_k, 0, wide)
        arrive(step, *faces[2])
        add(step, far_k, long_k, 0, wide)
        arrive(step, *faces[0])
        value = closed(step, first_k, short_k, 0, wide)
        finish(step + 1, *faces[0], value[:, :FACE_SHORT])
        finish(step + 1, *faces[1], value[:, FACE_SHORT:])
        value = closed(step, second_k, long_k + 2 * short_k, wide, wide)
        finish(step + 1, *faces[2], value[:, :FACE_LONG])
        rest = closed(step, second_k, long_k + 2 * short_k, 2 * wide, total - 2 * wide)
        finish(step + 1, *faces[3], jnp.concatenate([value[:, FACE_LONG:], rest], axis=1))
        if step == 0:
            for n in range(chunks):
                turn(n, blocks[:1])

    for step in (ITERS - 1, ITERS):
        for face in faces:
            send(step, *face, False)
    for face in faces[::-1]:
        receive(ITERS, *face)


def write_out(out_ref, in_ref, out_hbm, in_hbm, sem):
    copies = [pltpu.make_async_copy(out_ref, out_hbm.at[0, 0], sem.at[0]),
              pltpu.make_async_copy(in_ref, in_hbm.at[0, 0], sem.at[1])]
    for copy in copies:
        copy.start()
    for copy in copies:
        copy.wait()


def body(n_wide, n_narrow, operator, sources, face_lengths):
    total, width = sources.shape[2:]
    dtype = sources.dtype
    held = pltpu.VMEM((total, width), dtype)
    outgoing, incoming = pl.pallas_call(
        functools.partial(kernel, n_wide, n_narrow),
        out_shape=(held, held),
        in_specs=[
            pl.BlockSpec(memory_space=pltpu.HBM),
            pl.BlockSpec(memory_space=pltpu.HBM),
            pl.BlockSpec(memory_space=pltpu.HBM),
        ],
        out_specs=[pl.BlockSpec(memory_space=pltpu.VMEM)] * 2,
        scratch_shapes=[
            pltpu.VMEM((2, total, total), dtype),
            pltpu.VMEM((2 * total, total), dtype),
            pltpu.VMEM((total, width), dtype),
            pltpu.VMEM((width, total), dtype),
            pltpu.VMEM((total, width), dtype),
            pltpu.VMEM((ITERS, width, 2 * total), dtype),
            pltpu.VMEM((width, total), jnp.float32),
            pltpu.VMEM((ITERS - 1, 2, width, FACE_LONG), dtype),
            pltpu.VMEM((ITERS - 1, 2, width, FACE_SHORT), dtype),
            pltpu.SMEM((4,), jnp.int32),
            pltpu.SemaphoreType.DMA((total // CHUNK,)),
            pltpu.SemaphoreType.DMA,
            pltpu.SemaphoreType.DMA,
            pltpu.SemaphoreType.DMA((ITERS + 1, 4)),
            pltpu.SemaphoreType.DMA((ITERS + 1, 4)),
        ],
        compiler_params=pltpu.CompilerParams(
            collective_id=0, has_side_effects=True, vmem_limit_bytes=54 * 1024 * 1024),
        name="schwarz",
    )(operator, sources, face_lengths)
    shape = jax.ShapeDtypeStruct(sources.shape, dtype)
    return pl.pallas_call(
        write_out,
        out_shape=(shape, shape),
        in_specs=[pl.BlockSpec(memory_space=pltpu.VMEM)] * 2,
        out_specs=[pl.BlockSpec(memory_space=pl.ANY)] * 2,
        scratch_shapes=[pltpu.SemaphoreType.DMA((2,))],
        compiler_params=pltpu.CompilerParams(vmem_limit_bytes=4 * 1024 * 1024),
        name="write_out",
    )(outgoing, incoming)


def solution(mesh):
    in_specs = (
        P("wide", "narrow", None, None, None),
        P("wide", "narrow", None, None),
        P("wide", "narrow", None),
    )
    out_specs = (P("wide", "narrow", None, None), P("wide", "narrow", None, None))
    step = functools.partial(body, mesh.shape["wide"], mesh.shape["narrow"])
    return jax.shard_map(step, mesh=mesh, in_specs=in_specs, out_specs=out_specs, check_vma=False)
```
